32 devices in a mesh: train: 4 (over z), serve: 8 (over y, x, core).
Axes of the slice: x: 2, y: 2, z: 4, core: 2. Of those that a mesh axis runs over, the one named last changes fastest.
Arguments:
- train_weights: bfloat16 [16, 7424, 2112], P(None, 'train', 'serve'), may hold values from -6 to 6
- row_offset: int32 [16, 5], replicated, may hold values from 0 to 7168, as said below
- block_group: int32 [16, 224, 1], P(None, 'train'), may hold values from 0 to 7; in each aligned block of 56 rows (0 to 55, 56 to 111, ..., all dimensions but the last counted through in order) at most 8 rows name the same one
Outputs:
- quant_codes: bfloat16 [16, 8, 4, 8, 32, 2112], P(None, 'serve', 'train')
- block_scales: float32 [16, 8, 4, 8, 2112], P(None, 'serve', 'train')
The draws below stay inside these ranges and needn't reach their ends.
Inputs may be any that keep to these rules, and one draw needn't show every extreme that they name: For every layer l: row_offset[l, 0] = 0 and row_offset[l, 4] = 7168; every other row_offset[l, t] lies 1 to 32 rows above or below t * 1792, never on it; in every layer one entry lies exactly 32 rows above and another exactly 32 rows below; layer 1 has the opposite sign of layer 0 at every such entry. `block_group`: within each aligned block of 56 entries (one training device's blocks of one layer), no group is named more than 8 times; some group reaches 8 in some of them.
All inputs are finite; a program needn't handle non-finite values.
Results may differ from the reference program's by a relative error of at most 0.001.
Values may be sent and summed in bfloat16 or wider, within the bound.
A program may use at most 128 MiB of HBM per device.

```python
import math
import jax
import jax.numpy as jnp
import numpy as np
from jax import lax

MODEL_DIM = 7168
LAYERS = 16
BLOCK = 32
SHIFT = 32
FEAT = 2112
ROWS_DEV = 1792
SLOT = 1856
BLOCKS = 224
BLOCKS_DEV = 56
SLOTS = 8
N_TRAIN = 4
N_SERVE = 8


def draw_train_weights(key, part):
    base_key = jax.random.fold_in(key, 23)
    value_key, quiet_key, scale_key = jax.random.split(base_key, 3)
    full_shape = (LAYERS, N_TRAIN * SLOT, FEAT)
    values = jnp.clip(jax.random.normal(value_key, full_shape, jnp.float32), -6.0, 6.0)
    quiet_mask = jax.random.randint(quiet_key, (LAYERS, MODEL_DIM // BLOCK, FEAT), 0, 8, dtype=jnp.int32) == 0
    buffer_row = jnp.arange(N_TRAIN * SLOT, dtype=jnp.int32)
    owner_dev = buffer_row // SLOT
    global_row = jnp.clip(owner_dev * ROWS_DEV + buffer_row % SLOT - SHIFT, 0, MODEL_DIM - 1).astype(jnp.int32)
    block_of_row = (global_row // BLOCK).astype(jnp.int32)
    quiet_rows = jnp.take(quiet_mask, block_of_row, axis=1)
    damping = jnp.where(quiet_rows, 0.02, 1.0).astype(jnp.float32)
    return (values * damping).astype(jnp.bfloat16)


def draw_row_offset(key, part):
    base_key = jax.random.fold_in(key, 11)
    size_key, sign_key, pick_key = jax.random.split(base_key, 3)
    magnitude = jax.random.randint(size_key, (LAYERS, N_TRAIN - 1), 1, SHIFT + 1, dtype=jnp.int32)
    signs = jax.random.randint(sign_key, (LAYERS, N_TRAIN - 1), 0, 2, dtype=jnp.int32) * 2 - 1
    inner = (magnitude * signs).astype(jnp.int32)
    pick_keys = jax.random.split(pick_key, LAYERS)
    picked = jax.vmap(lambda one_key: jax.random.permutation(one_key, N_TRAIN - 1))(pick_keys)
    column_ids = jnp.arange(N_TRAIN - 1, dtype=jnp.int32)[None, :]
    inner = jnp.where(column_ids == picked[:, 0:1], SHIFT, inner)
    inner = jnp.where(column_ids == picked[:, 1:2], -SHIFT, inner)
    layer_ids = jnp.arange(LAYERS, dtype=jnp.int32)[:, None]
    inner = jnp.where(layer_ids == 1, -inner[0:1], inner).astype(jnp.int32)
    middle = jnp.arange(1, N_TRAIN, dtype=jnp.int32)[None, :] * ROWS_DEV + inner
    start = jnp.zeros((LAYERS, 1), jnp.int32)
    finish = jnp.full((LAYERS, 1), N_TRAIN * ROWS_DEV, jnp.int32)
    return jnp.concatenate([start, middle, finish], axis=1).astype(jnp.int32)


def routed_block(key, own, number, rows, number_of, top, most, slope):
    order = jax.random.permutation(key, number_of)
    crowded, ordinary = shares(number_of, rows * top, most, slope, True), shares(number_of, rows * top, most, slope, False)
    places = jnp.arange(number_of)

    def named(lengths, rotation):
        used = int((lengths > 0).sum())
        fixed = max(1, used // 4)
        moved = fixed + (places - fixed + rotation * (used - fixed)) % max(1, number_of - fixed)
        return jnp.zeros((number_of,), jnp.int32).at[order[jnp.where(places < fixed, places, moved)]].set(jnp.asarray(lengths, jnp.int32))

    lengths = jnp.where(number % 4 == 0, named(crowded, number // 4), named(ordinary, number - number // 4 - 1))
    mixed = jax.random.permutation(jax.random.fold_in(own, 3), number_of)
    donor, sink = mixed[0:number_of // 2 * 2:2], mixed[1:number_of // 2 * 2:2]
    slack = jnp.minimum(lengths[donor] - 1, most - lengths[sink]) // 2
    slack = jnp.where((donor == order[0]) | (sink == order[0]) | (lengths[sink] == 0), 0, jnp.maximum(slack, 0))
    moved = jax.random.randint(jax.random.fold_in(own, 4), (number_of // 2,), 0, 1 << 20) % (slack + 1)
    lengths = lengths.at[donor].add(-moved).at[sink].add(moved)
    labels = jnp.searchsorted(jnp.cumsum(lengths), jnp.arange(rows * top), side="right").astype(jnp.int32)
    listing = labels.reshape(top, rows).T
    listing = listing[jax.random.permutation(jax.random.fold_in(own, 1), rows)]
    rotation = jax.random.randint(jax.random.fold_in(own, 2), (rows, 1), 0, top)
    return jnp.take_along_axis(listing, (jnp.arange(top)[None, :] + rotation) % top, axis=1)


def shares(number_of, total, bound, skew, full):
    portions = [(1 << 20) // math.isqrt(grade ** skew) + 1 for grade in range(1, number_of + 1)]
    largest = bound if full else min(bound, max(-(-total // number_of), total * portions[0] // sum(portions)))
    least = 1 if total - largest >= number_of - 1 else 0
    given, rest = [largest] + [least] * (number_of - 1), total - largest - least * (number_of - 1)
    while rest > 0:
        movable = [i for i in range(1, number_of) if given[i] < largest] or [i for i in range(1, number_of) if given[i] < bound]
        pool, budget = sum([portions[i] for i in movable]), rest
        for i in movable:
            extra = min(bound - given[i], max(1, budget * portions[i] // pool), rest)
            given[i] = given[i] + extra
            rest = rest - extra
    return np.array(given)


def setup_inputs(seed: int = 0) -> dict:
    splits = jax.random.split(jax.random.key(seed), 4)
    train_weights = draw_train_weights(jax.random.fold_in(splits[3], 71), 0)
    row_offset = draw_row_offset(jax.random.fold_in(splits[3], 71), 0)
    block_group_keys = jax.random.split(jax.random.fold_in(splits[2], 1), LAYERS * BLOCKS // BLOCKS_DEV)
    block_group_turns = jax.random.permutation(jax.random.fold_in(splits[2], 3), LAYERS * BLOCKS // BLOCKS_DEV)
    block_group = jax.vmap(lambda own, number: routed_block(jax.random.fold_in(splits[2], 2), own, number, BLOCKS_DEV, N_SERVE, 1, SLOTS, 0))(block_group_keys, block_group_turns).reshape((LAYERS, BLOCKS, 1))
    return {"train_weights": train_weights, "row_offset": row_offset, "block_group": block_group}


def reference(train_weights, row_offset, block_group):
    row_ids = jnp.arange(MODEL_DIM, dtype=jnp.int32)
    block_owner = (jnp.arange(BLOCKS, dtype=jnp.int32) // BLOCKS_DEV).astype(jnp.int32)
    position = jnp.arange(BLOCKS_DEV, dtype=jnp.int32)
    earlier = position[None, :] < position[:, None]

    def one_layer(inputs):
        weights, groups, offsets = inputs
        owner_dev = jnp.sum((row_ids[:, None] >= offsets[None, 1:N_TRAIN]).astype(jnp.int32), axis=1).astype(jnp.int32)
        source = (owner_dev * SLOT + row_ids - owner_dev * ROWS_DEV + SHIFT).astype(jnp.int32)
        gathered = jnp.take(weights, source, axis=0)
        blocks = gathered.reshape(BLOCKS, BLOCK, FEAT).astype(jnp.float32)
        absmax = jnp.max(jnp.abs(blocks), axis=1)
        divisor = jnp.maximum(absmax, 0.25)
        coded = (blocks / divisor[:, None, :]).astype(jnp.bfloat16)
        group_ids = groups[:, 0].astype(jnp.int32)
        per_dev = group_ids.reshape(N_TRAIN, BLOCKS_DEV)
        same_group = per_dev[:, :, None] == per_dev[:, None, :]
        order_in = jnp.sum((same_group & earlier[None]).astype(jnp.int32), axis=2).reshape(BLOCKS).astype(jnp.int32)
        flat_slot = ((group_ids * N_TRAIN + block_owner) * SLOTS + order_in).astype(jnp.int32)
        out_codes = jnp.zeros((N_SERVE * N_TRAIN * SLOTS, BLOCK, FEAT), jnp.bfloat16).at[flat_slot].set(coded)
        out_scales = jnp.zeros((N_SERVE * N_TRAIN * SLOTS, FEAT), jnp.float32).at[flat_slot].set(divisor)
        return (out_codes.reshape(N_SERVE, N_TRAIN, SLOTS, BLOCK, FEAT),
                out_scales.reshape(N_SERVE, N_TRAIN, SLOTS, FEAT))

    quant_codes, block_scales = lax.map(one_layer, (train_weights, block_group, row_offset))
    return quant_codes, block_scales
```

```python
import functools

import jax
import jax.numpy as jnp
from jax import lax
from jax.experimental import pallas as pl
from jax.experimental.pallas import tpu as pltpu
from jax.sharding import PartitionSpec as P

BLOCK = 32
SHIFT = 32
LANES = 128
PAIR = 2
CHUNKS = 4


def turned(values):
    return jnp.transpose(values.astype(jnp.float32))


def pack_kernel(base, slots_n, group_ref, order_ref, first_ref, next_ref, wt_ref, left_ref, right_ref, out_ref, rem_ref, w_ref):
    step = pl.program_id(0)
    columns, buffer_len = wt_ref.shape[1:]
    full = columns // LANES
    rem = columns - full * LANES
    blocks_dev = group_ref.shape[1]
    groups = out_ref.shape[0]
    row = lax.broadcasted_iota(jnp.int32, (BLOCK, columns), 0)
    for sub in range(PAIR):
        layer = (base + step) * PAIR + sub
        for low in range(0, buffer_len, LANES):
            high = min(low + LANES, buffer_len)
            w_ref[sub, low:high, :] = turned(wt_ref[sub, :, low:high]).astype(w_ref.dtype)

        def place(j, block, sub=sub, layer=layer):
            g = group_ref[layer, j]
            k = order_ref[layer, j]
            for t in range(full):
                out_ref[g, 0, (sub * slots_n + k) * full + t] = block[:, t * LANES : (t + 1) * LANES]
            if rem:
                rem_ref[g, sub * slots_n + k, :, 0:rem] = block[:, full * LANES :]

        def inner(j, carry, sub=sub, place=place):
            start = pl.multiple_of(SHIFT + j * BLOCK, BLOCK)
            place(j, w_ref[sub, pl.ds(start, BLOCK), :])
            return carry

        lax.fori_loop(1, blocks_dev - 1, inner, 0, unroll=6 if (blocks_dev - 2) % 6 == 0 else 2)
        head = jnp.where(
            row < first_ref[layer],
            left_ref[sub].astype(jnp.float32),
            w_ref[sub, SHIFT : SHIFT + BLOCK, :].astype(jnp.float32),
        )
        place(0, head.astype(out_ref.dtype))
        last = (blocks_dev - 1) * BLOCK
        tail = jnp.where(
            row + last >= next_ref[layer],
            right_ref[sub].astype(jnp.float32),
            w_ref[sub, SHIFT + last : SHIFT + last + BLOCK, :].astype(jnp.float32),
        )
        place(blocks_dev - 1, tail.astype(out_ref.dtype))
    if rem:
        lane = lax.broadcasted_iota(jnp.int32, (BLOCK, LANES), 1)

        def gather(g, carry):
            tile = rem_ref[g, 0].astype(jnp.float32)
            for i in range(1, PAIR * slots_n):
                moved = pltpu.roll(rem_ref[g, i].astype(jnp.float32), i * rem, 1)
                tile = jnp.where(lane >= i * rem, moved, tile)
            out_ref[g, 0, PAIR * slots_n * full] = tile.astype(out_ref.dtype)
            return carry

        lax.fori_loop(0, groups, gather, 0)


def unpack_kernel(base, slots_n, columns, count_ref, *refs):
    recv_ref, codes_ref, scale_ref, rem_code, rem_scale = refs[0], *refs[-4:]
    step = pl.program_id(0)
    full = columns // LANES
    rem = columns - full * LANES
    sources = recv_ref.shape[0]
    width = codes_ref.shape[3]
    tiles = -(-width // LANES)

    def scaled(values):
        values = values.astype(jnp.float32)
        divisor = jnp.maximum(jnp.max(jnp.abs(values), axis=0, keepdims=True), 0.25)
        return values * (1.0 / divisor), divisor

    if rem:
        for s in range(sources):
            rem_code[s], rem_scale[s] = scaled(recv_ref[s, 0, PAIR * slots_n * full])
    lane = lax.broadcasted_iota(jnp.int32, (BLOCK, LANES), 1)
    lane_row = lax.broadcasted_iota(jnp.int32, (1, LANES), 1)

    for sub in range(PAIR):
        count = count_ref[(base + step) * PAIR + sub]
        for k in range(slots_n):
            i = sub * slots_n + k

            @pl.when(k < count)
            def _():
                parts = [None] * tiles

                def put(tile, low, code, scale):
                    if tile >= tiles:
                        return
                    if parts[tile] is None:
                        parts[tile] = (code, scale)
                    else:
                        before = parts[tile]
                        parts[tile] = (
                            jnp.where(lane >= low, code, before[0]),
                            jnp.where(lane_row >= low, scale, before[1]),
                        )

                def flush(below):
                    for tile in range(below):
                        if parts[tile] is not None:
                            code, scale = parts[tile]
                            end = min(width, (tile + 1) * LANES)
                            size = end - tile * LANES
                            codes_ref[sub, k, :, tile * LANES : end] = code[:, :size].astype(codes_ref.dtype)
                            scale_ref[sub, k : k + 1, tile * LANES : end] = scale[:, :size]
                            parts[tile] = None

                for s in range(sources):
                    for t in range(full + (1 if rem else 0)):
                        start = s * columns + t * LANES
                        size = LANES if t < full else rem
                        low = start % LANES
                        if t < full:
                            code, scale = scaled(recv_ref[s, 0, i * full + t])
                            turn = low
                        else:
                            code, scale = rem_code[s], rem_scale[s]
                            turn = (low - i * rem) % LANES
                        if turn:
                            code = pltpu.roll(code, turn, 1)
                            scale = pltpu.roll(scale, turn, 1)
                        tile = start // LANES
                        put(tile, low, code, scale)
                        if low + size > LANES:
                            put(tile + 1, 0, code, scale)
                        flush((start + size) // LANES)
                flush(tiles)

            @pl.when(k >= count)
            def _():
                codes_ref[sub, k] = jnp.zeros((BLOCK, width), codes_ref.dtype)
                scale_ref[sub, k : k + 1] = jnp.zeros((1, width), scale_ref.dtype)


def shards(train_weights, row_offset, block_group):
    train_n = lax.axis_size("train")
    serve_n = lax.axis_size("serve")
    train_idx = lax.axis_index("train")
    serve_idx = lax.axis_index("serve")
    layers, buffer_len, columns = train_weights.shape
    rows_dev = buffer_len - 2 * SHIFT
    blocks_dev = block_group.shape[1]
    slots_n = (blocks_dev + serve_n - 1) // serve_n + 1
    full = columns // LANES
    rem = columns - full * LANES
    assert PAIR * slots_n * rem <= LANES and layers % PAIR == 0
    pieces = PAIR * slots_n * full + (1 if rem else 0)
    pairs = layers // PAIR
    chunks = CHUNKS if pairs % CHUNKS == 0 else 1
    per = pairs // chunks
    width = columns * serve_n
    dtype = train_weights.dtype

    entries = jnp.arange(train_n + 1, dtype=jnp.int32)
    position = jnp.arange(blocks_dev, dtype=jnp.int32)
    earlier = position[None, :] < position[:, None]
    group_ids = block_group[:, :, 0]
    first_row = jnp.sum(jnp.where(entries[None, :] == train_idx, row_offset, 0), axis=1) - train_idx * rows_dev
    next_row = jnp.sum(jnp.where(entries[None, :] == train_idx + 1, row_offset, 0), axis=1) - train_idx * rows_dev
    same_group = group_ids[:, :, None] == group_ids[:, None, :]
    order_in = jnp.sum((same_group & earlier[None]).astype(jnp.int32), axis=2)
    count = jnp.sum((group_ids == serve_idx).astype(jnp.int32), axis=1)

    ends = train_n - 1
    up = [(i, i + 1) for i in range(ends)]
    down = [(i + 1, i) for i in range(ends)]
    turned_weights = jnp.swapaxes(train_weights, 1, 2)
    received = []
    for c in range(chunks):
        low, high = c * per * PAIR, (c + 1) * per * PAIR
        left = lax.ppermute(train_weights[low:high, buffer_len - SHIFT :], "train", up)
        right = lax.ppermute(train_weights[low:high, :SHIFT], "train", down)
        sent = pl.pallas_call(
            functools.partial(pack_kernel, c * per, slots_n),
            grid_spec=pltpu.PrefetchScalarGridSpec(
                num_scalar_prefetch=4,
                grid=(per,),
                in_specs=[
                    pl.BlockSpec((PAIR, columns, buffer_len), lambda p, *_, c=c: (c * per + p, 0, 0)),
                    pl.BlockSpec((PAIR, SHIFT, columns), lambda p, *_: (p, 0, 0)),
                    pl.BlockSpec((PAIR, SHIFT, columns), lambda p, *_: (p, 0, 0)),
                ],
                out_specs=pl.BlockSpec((serve_n, 1, pieces, BLOCK, LANES), lambda p, *_: (0, p, 0, 0, 0)),
                scratch_shapes=[pltpu.VMEM((serve_n, PAIR * slots_n, BLOCK, LANES), dtype), pltpu.VMEM((PAIR, buffer_len, columns), dtype)],
            ),
            out_shape=jax.ShapeDtypeStruct((serve_n, per, pieces, BLOCK, LANES), dtype),
            cost_estimate=pl.CostEstimate(flops=0, bytes_accessed=30_000_000 // chunks, transcendentals=0),
            name=f"pack{c}",
        )(group_ids, order_in, first_row, next_row, turned_weights, left, right)
        received.append(lax.all_to_all(sent, "serve", split_axis=0, concat_axis=0, tiled=True))

    outs = None
    for c in range(chunks):
        held = () if outs is None else outs
        outs = pl.pallas_call(
            functools.partial(unpack_kernel, c * per, slots_n, columns),
            grid_spec=pltpu.PrefetchScalarGridSpec(
                num_scalar_prefetch=1,
                grid=(per,),
                in_specs=[pl.BlockSpec((serve_n, 1, pieces, BLOCK, LANES), lambda p, *_: (0, p, 0, 0, 0))]
                + [pl.BlockSpec(memory_space=pl.ANY)] * len(held),
                out_specs=[
                    pl.BlockSpec((PAIR, slots_n, BLOCK, width), lambda p, *_, c=c: (c * per + p, 0, 0, 0)),
                    pl.BlockSpec((PAIR, slots_n, width), lambda p, *_, c=c: (c * per + p, 0, 0)),
                ],
                scratch_shapes=[
                    pltpu.VMEM((serve_n, BLOCK, LANES), jnp.float32),
                    pltpu.VMEM((serve_n, 1, LANES), jnp.float32),
                ],
            ),
            out_shape=[
                jax.ShapeDtypeStruct((layers, slots_n, BLOCK, width), dtype),
                jax.ShapeDtypeStruct((layers, slots_n, width), jnp.float32),
            ],
            input_output_aliases={2: 0, 3: 1} if held else {},
            cost_estimate=pl.CostEstimate(flops=0, bytes_accessed=40_000_000 // chunks, transcendentals=0),
            name=f"unpack{c}",
        )(count, received[c], *held)
    codes, scales = outs
    return (
        codes.reshape(layers, 1, 1, slots_n, BLOCK, width),
        scales.reshape(layers, 1, 1, slots_n, width),
    )


def solution(mesh):
    return jax.shard_map(
        shards,
        mesh=mesh,
        in_specs=(P(None, "train", "serve"), P(), P(None, "train", None)),
        out_specs=(
            P(None, "serve", "train", None, None, None),
            P(None, "serve", "train", None, None),
        ),
        check_vma=False,
    )
```

```python
import functools

import jax
import jax.numpy as jnp
from jax import lax
from jax.experimental import pallas as pl
from jax.experimental.pallas import tpu as pltpu
from jax.sharding import PartitionSpec as P

BLOCK = 32
SHIFT = 32
LANES = 128
PAIR = 2


def turned(values):
    return jnp.transpose(values.astype(jnp.float32))


def pack_kernel(base, slots_n, group_ref, order_ref, first_ref, next_ref, wt_ref, left_ref, right_ref, *refs):
    out_ref, rem_ref, w_ref = refs[-3:]
    step = pl.program_id(0)
    columns, buffer_len = wt_ref.shape[1:]
    full = columns // LANES
    rem = columns - full * LANES
    blocks_dev = group_ref.shape[1]
    groups = out_ref.shape[0]
    row = lax.broadcasted_iota(jnp.int32, (BLOCK, columns), 0)
    for sub in range(PAIR):
        layer = (base + step) * PAIR + sub
        for low in range(0, buffer_len, LANES):
            high = min(low + LANES, buffer_len)
            w_ref[sub, low:high, :] = turned(wt_ref[sub, :, low:high]).astype(w_ref.dtype)

        def place(j, block, sub=sub, layer=layer):
            g = group_ref[layer, j]
            k = order_ref[layer, j]
            for t in range(full):
                out_ref[g, 0, (sub * slots_n + k) * full + t] = block[:, t * LANES : (t + 1) * LANES]
            if rem:
                rem_ref[g, sub * slots_n + k, :, 0:rem] = block[:, full * LANES :]

        def inner(j, carry, sub=sub, place=place):
            start = pl.multiple_of(SHIFT + j * BLOCK, BLOCK)
            place(j, w_ref[sub, pl.ds(start, BLOCK), :])
            return carry

        lax.fori_loop(1, blocks_dev - 1, inner, 0, unroll=6 if (blocks_dev - 2) % 6 == 0 else 2)
        head = jnp.where(
            row < first_ref[layer],
            left_ref[sub].astype(jnp.float32),
            w_ref[sub, SHIFT : SHIFT + BLOCK, :].astype(jnp.float32),
        )
        place(0, head.astype(out_ref.dtype))
        last = (blocks_dev - 1) * BLOCK
        tail = jnp.where(
            row + last >= next_ref[layer],
            right_ref[sub].astype(jnp.float32),
            w_ref[sub, SHIFT + last : SHIFT + last + BLOCK, :].astype(jnp.float32),
        )
        place(blocks_dev - 1, tail.astype(out_ref.dtype))
    if rem:
        lane = lax.broadcasted_iota(jnp.int32, (BLOCK, LANES), 1)

        def gather(g, carry):
            tile = rem_ref[g, 0].astype(jnp.float32)
            for i in range(1, PAIR * slots_n):
                moved = pltpu.roll(rem_ref[g, i].astype(jnp.float32), i * rem, 1)
                tile = jnp.where(lane >= i * rem, moved, tile)
            out_ref[g, 0, PAIR * slots_n * full] = tile.astype(out_ref.dtype)
            return carry

        lax.fori_loop(0, groups, gather, 0)


def unpack_kernel(base, slots_n, columns, count_ref, *refs):
    recv_ref, codes_ref, scale_ref, rem_code, rem_scale = refs[0], *refs[-4:]
    step = pl.program_id(0)
    full = columns // LANES
    rem = columns - full * LANES
    sources = recv_ref.shape[0]
    width = codes_ref.shape[3]
    tiles = -(-width // LANES)

    def scaled(values):
        values = values.astype(jnp.float32)
        divisor = jnp.maximum(jnp.max(jnp.abs(values), axis=0, keepdims=True), 0.25)
        return values * (1.0 / divisor), divisor

    if rem:
        for s in range(sources):
            rem_code[s], rem_scale[s] = scaled(recv_ref[s, 0, PAIR * slots_n * full])
    lane = lax.broadcasted_iota(jnp.int32, (BLOCK, LANES), 1)
    lane_row = lax.broadcasted_iota(jnp.int32, (1, LANES), 1)

    for sub in range(PAIR):
        count = count_ref[(base + step) * PAIR + sub]
        for k in range(slots_n):
            i = sub * slots_n + k

            @pl.when(k < count)
            def _():
                parts = [None] * tiles

                def put(tile, low, code, scale):
                    if tile >= tiles:
                        return
                    if parts[tile] is None:
                        parts[tile] = (code, scale)
                    else:
                        before = parts[tile]
                        parts[tile] = (
                            jnp.where(lane >= low, code, before[0]),
                            jnp.where(lane_row >= low, scale, before[1]),
                        )

                def flush(below):
                    for tile in range(below):
                        if parts[tile] is not None:
                            code, scale = parts[tile]
                            end = min(width, (tile + 1) * LANES)
                            size = end - tile * LANES
                            codes_ref[sub, k, :, tile * LANES : end] = code[:, :size].astype(codes_ref.dtype)
                            scale_ref[sub, k : k + 1, tile * LANES : end] = scale[:, :size]
                            parts[tile] = None

                for s in range(sources):
                    for t in range(full + (1 if rem else 0)):
                        start = s * columns + t * LANES
                        size = LANES if t < full else rem
                        low = start % LANES
                        if t < full:
                            code, scale = scaled(recv_ref[s, 0, i * full + t])
                            turn = low
                        else:
                            code, scale = rem_code[s], rem_scale[s]
                            turn = (low - i * rem) % LANES
                        if turn:
                            code = pltpu.roll(code, turn, 1)
                            scale = pltpu.roll(scale, turn, 1)
                        tile = start // LANES
                        put(tile, low, code, scale)
                        if low + size > LANES:
                            put(tile + 1, 0, code, scale)
                        flush((start + size) // LANES)
                flush(tiles)

            @pl.when(k >= count)
            def _():
                codes_ref[sub, k] = jnp.zeros((BLOCK, width), codes_ref.dtype)
                scale_ref[sub, k : k + 1] = jnp.zeros((1, width), scale_ref.dtype)


def shards(train_weights, row_offset, block_group):
    train_n = lax.axis_size("train")
    serve_n = lax.axis_size("serve")
    train_idx = lax.axis_index("train")
    serve_idx = lax.axis_index("serve")
    layers, buffer_len, columns = train_weights.shape
    rows_dev = buffer_len - 2 * SHIFT
    blocks_dev = block_group.shape[1]
    slots_n = (blocks_dev + serve_n - 1) // serve_n + 1
    full = columns // LANES
    rem = columns - full * LANES
    assert PAIR * slots_n * rem <= LANES and layers % PAIR == 0
    pieces = PAIR * slots_n * full + (1 if rem else 0)
    pairs = layers // PAIR
    ends = [max(1, pairs // 4), max(1, pairs // 8)]
    sizes = [ends[0], pairs - sum(ends), ends[1]] if pairs > sum(ends) else [pairs]
    firsts = [sum(sizes[:c]) for c in range(len(sizes))]
    width = columns * serve_n
    dtype = train_weights.dtype

    entries = jnp.arange(train_n + 1, dtype=jnp.int32)
    position = jnp.arange(blocks_dev, dtype=jnp.int32)
    earlier = position[None, :] < position[:, None]
    group_ids = block_group[:, :, 0]
    first_row = jnp.sum(jnp.where(entries[None, :] == train_idx, row_offset, 0), axis=1) - train_idx * rows_dev
    next_row = jnp.sum(jnp.where(entries[None, :] == train_idx + 1, row_offset, 0), axis=1) - train_idx * rows_dev
    same_group = group_ids[:, :, None] == group_ids[:, None, :]
    order_in = jnp.sum((same_group & earlier[None]).astype(jnp.int32), axis=2)
    count = jnp.sum((group_ids == serve_idx).astype(jnp.int32), axis=1)

    up = [(i, i + 1) for i in range(train_n - 1)]
    down = [(i + 1, i) for i in range(train_n - 1)]
    turned_weights = jnp.swapaxes(train_weights, 1, 2)

    def pack(c, after):
        base, per = firsts[c], sizes[c]
        low, high = base * PAIR, (base + per) * PAIR
        left = lax.ppermute(train_weights[low:high, buffer_len - SHIFT :], "train", up)
        right = lax.ppermute(train_weights[low:high, :SHIFT], "train", down)
        sent = pl.pallas_call(
            functools.partial(pack_kernel, base, slots_n),
            grid_spec=pltpu.PrefetchScalarGridSpec(
                num_scalar_prefetch=4,
                grid=(per,),
                in_specs=[
                    pl.BlockSpec((PAIR, columns, buffer_len), lambda p, *_: (base + p, 0, 0)),
                    pl.BlockSpec((PAIR, SHIFT, columns), lambda p, *_: (p, 0, 0)),
                    pl.BlockSpec((PAIR, SHIFT, columns), lambda p, *_: (p, 0, 0)),
                ]
                + [pl.BlockSpec(memory_space=pl.ANY)] * len(after),
                out_specs=pl.BlockSpec((serve_n, 1, pieces, BLOCK, LANES), lambda p, *_: (0, p, 0, 0, 0)),
                scratch_shapes=[
                    pltpu.VMEM((serve_n, PAIR * slots_n, BLOCK, LANES), dtype),
                    pltpu.VMEM((PAIR, buffer_len, columns), dtype),
                ],
            ),
            out_shape=jax.ShapeDtypeStruct((serve_n, per, pieces, BLOCK, LANES), dtype),
            cost_estimate=pl.CostEstimate(flops=0, bytes_accessed=12_000_000 * per, transcendentals=0),
            name=f"pack{c}",
        )(group_ids, order_in, first_row, next_row, turned_weights, left, right, *after)
        return lax.all_to_all(sent, "serve", split_axis=0, concat_axis=0, tiled=True)

    def unpack(c, received, held):
        base, per = firsts[c], sizes[c]
        return pl.pallas_call(
            functools.partial(unpack_kernel, base, slots_n, columns),
            grid_spec=pltpu.PrefetchScalarGridSpec(
                num_scalar_prefetch=1,
                grid=(per,),
                in_specs=[pl.BlockSpec((serve_n, 1, pieces, BLOCK, LANES), lambda p, *_: (0, p, 0, 0, 0))]
                + [pl.BlockSpec(memory_space=pl.ANY)] * len(held),
                out_specs=[
                    pl.BlockSpec((PAIR, slots_n, BLOCK, width), lambda p, *_: (base + p, 0, 0, 0)),
                    pl.BlockSpec((PAIR, slots_n, width), lambda p, *_: (base + p, 0, 0)),
                ],
                scratch_shapes=[
                    pltpu.VMEM((serve_n, BLOCK, LANES), jnp.float32),
                    pltpu.VMEM((serve_n, 1, LANES), jnp.float32),
                ],
            ),
            out_shape=[
                jax.ShapeDtypeStruct((layers, slots_n, BLOCK, width), dtype),
                jax.ShapeDtypeStruct((layers, slots_n, width), jnp.float32),
            ],
            input_output_aliases={2: 0, 3: 1} if held else {},
            cost_estimate=pl.CostEstimate(flops=0, bytes_accessed=12_000_000 * per, transcendentals=0),
            compiler_params=pltpu.CompilerParams(vmem_limit_bytes=24 * 1024 * 1024),
            name=f"unpack{c}",
        )(count, received, *held)

    outs, received = (), []
    for c in range(len(sizes)):
        if c >= 2:
            outs = unpack(c - 2, received[c - 2], outs)
        received.append(pack(c, outs[1:]))
    for c in range(max(0, len(sizes) - 2), len(sizes)):
        outs = unpack(c, received[c], outs)
    codes, scales = outs
    return (
        codes.reshape(layers, 1, 1, slots_n, BLOCK, width),
        scales.reshape(layers, 1, 1, slots_n, width),
    )


def solution(mesh):
    return jax.shard_map(
        shards,
        mesh=mesh,
        in_specs=(P(None, "train", "serve"), P(), P(None, "train", None)),
        out_specs=(
            P(None, "serve", "train", None, None, None),
            P(None, "serve", "train", None, None),
        ),
        check_vma=False,
    )
```
